32 devices in a mesh: group: 1, ctx: 32 (over z, y, x, core).
Axes of the slice: x: 2, y: 2, z: 4, core: 2. Of those that a mesh axis runs over, the one named last changes fastest.
Arguments:
- queries: bfloat16 [2, 64, 128], P('group'), may hold values from -80 to 80
- key_cache: bfloat16 [2, 4096, 512], P('group', 'ctx'), may hold values from -4 to 4
- value_cache: bfloat16 [2, 4096, 512], P('group', 'ctx'), may hold values from -6 to 6
- out_weight: bfloat16 [8192, 4096], P('ctx'), may hold values from -0.125 to 0.125
- hidden_in: bfloat16 [2, 4096], P('group'), may hold values from -45 to 45
- norm_gain: float32 [4096], replicated, may hold values from 0.25 to 1.75
- gate_weight: bfloat16 [32, 4096, 192], P('ctx'), may hold values from -0.09375 to 0.09375
- up_weight: bfloat16 [32, 4096, 192], P('ctx'), may hold values from -0.09375 to 0.09375
- down_weight: bfloat16 [32, 192, 4096], P('ctx'), may hold values from -0.15625 to 0.15625
- routes: int32 [2, 4], P('group'), may hold values from 0 to 3, all different within a row; in each aligned block of 2 rows (0 to 1, 2 to 3, ...) at most 2 rows name the same one
- route_weight: float32 [2, 4], P('group'), may hold values from 0.1 to 1
Outputs:
- mixed: float32 [2, 4096], P('group', 'ctx')
The draws below stay inside these ranges and needn't reach their ends.
Inputs may be any that keep to these rules, and one draw needn't show every extreme that they name: `routes`: each row names 4 different experts; no expert is named by more than 2 rows, a bound that some block reaches.
All inputs are finite; a program needn't handle non-finite values.
Results may differ from the reference program's by a relative error of at most 0.0035.
Values may be sent and summed in bfloat16 or wider, within the bound.
No kernel may reach another device: no remote copies, remote signals or barrier semaphores. Data moves between devices by JAX's collectives and lax.ppermute only.
A program may use at most 64 MiB of HBM per device.

```python
import math
import jax
import jax.numpy as jnp
import numpy as np
from jax import lax

D = 4096
HEADS = 64
KVH = 4
HD = 128
FF = 1536
QUARTERS = 8
TOP = 4
SEQS = 2
CONTEXT = 4096
EXPERTS = 4
SHARDS = 32
HID_DEV = 192
CAP = 2


def attention_pair(key):
    base_key = jax.random.fold_in(key, 17)
    key_q, key_k = jax.random.split(base_key, 2)
    key_vals = jnp.clip(jax.random.normal(key_k, (SEQS, CONTEXT, KVH, HD), jnp.float32), -4.0, 4.0)
    query_vals = jnp.clip(2.5 * jax.random.normal(key_q, (SEQS, HEADS, HD), jnp.float32), -10.0, 10.0)
    return (query_vals, key_vals.reshape(SEQS, CONTEXT, KVH * HD))


def draw_queries(key, part):
    return attention_pair(key)[0].astype(jnp.bfloat16)


def draw_key_cache(key, part):
    return attention_pair(key)[1].astype(jnp.bfloat16)


def draw_hidden_in(key, part):
    key_a = jax.random.fold_in(jax.random.fold_in(key, 29), 0)
    column = jnp.arange(D, dtype=jnp.float32) / D
    values = jnp.clip(jax.random.normal(key_a, (SEQS, D), jnp.float32), -4.0, 4.0) * jnp.power(3.0, column)[None, :] / math.sqrt(3.0)
    return values.astype(jnp.bfloat16)


def strengthened(drawn, rng, source, target, parts, factor):
    owner, partner = [(jnp.arange(drawn.shape[position]) // (drawn.shape[position] // parts)).reshape([-1 if axis == position else 1 for axis in range(drawn.ndim)]) for position in (source, target)]
    chosen = jax.random.permutation(rng, parts)[partner]
    strong = (owner == chosen) | (owner == (partner + parts // 2) % parts)
    return jnp.where(strong, factor * drawn, drawn)


def steps_of(key, shape, shards, smallest, largest):
    def one(position, blocks):
        heights = jax.random.uniform(jax.random.fold_in(jax.random.fold_in(key, 6), position), (blocks,), jnp.float32, smallest / len(shards), largest / len(shards))
        return jnp.repeat(jnp.exp(heights), shape[position] // blocks).reshape((-1,) + (1,) * (len(shape) - position - 1))

    factor_of = one(*shards[0])
    for cut in shards[1:]:
        factor_of = factor_of * one(*cut)
    return factor_of


def shared_out(stream_key, own, number, rows, count, top, most, slope):
    ranking = jax.random.permutation(stream_key, count)
    heavy_load, usual = load_shares(count, rows * top, most, slope, True), load_shares(count, rows * top, most, slope, False)
    places = jnp.arange(count)

    def named(tallies, turn):
        used = int((tallies > 0).sum())
        fixed = max(1, used // 4)
        shifted = fixed + (places - fixed + turn * (used - fixed)) % max(1, count - fixed)
        return jnp.zeros((count,), jnp.int32).at[ranking[jnp.where(places < fixed, places, shifted)]].set(jnp.asarray(tallies, jnp.int32))

    tallies = jnp.where(number % 4 == 0, named(heavy_load, number // 4), named(usual, number - number // 4 - 1))
    mixed = jax.random.permutation(jax.random.fold_in(own, 3), count)
    source_of, sink = mixed[0:count // 2 * 2:2], mixed[1:count // 2 * 2:2]
    margin = jnp.minimum(tallies[source_of] - 1, most - tallies[sink]) // 2
    margin = jnp.where((source_of == ranking[0]) | (sink == ranking[0]) | (tallies[sink] == 0), 0, jnp.maximum(margin, 0))
    shifted = jax.random.randint(jax.random.fold_in(own, 4), (count // 2,), 0, 1 << 20) % (margin + 1)
    tallies = tallies.at[source_of].add(-shifted).at[sink].add(shifted)
    items = jnp.searchsorted(jnp.cumsum(tallies), jnp.arange(rows * top), side="right").astype(jnp.int32)
    table = items.reshape(top, rows).T
    table = table[jax.random.permutation(jax.random.fold_in(own, 1), rows)]
    turn = jax.random.randint(jax.random.fold_in(own, 2), (rows, 1), 0, top)
    return jnp.take_along_axis(table, (jnp.arange(top)[None, :] + turn) % top, axis=1)


def load_shares(amount, total, limit, lean, full):
    weights = [(1 << 20) // math.isqrt(standing ** lean) + 1 for standing in range(1, amount + 1)]
    largest = limit if full else min(limit, max(-(-total // amount), total * weights[0] // sum(weights)))
    least = 1 if total - largest >= amount - 1 else 0
    counts, spare = [largest] + [least] * (amount - 1), total - largest - least * (amount - 1)
    while spare > 0:
        free = [i for i in range(1, amount) if counts[i] < largest] or [i for i in range(1, amount) if counts[i] < limit]
        mass, left = sum([weights[i] for i in free]), spare
        for i in free:
            addition = min(limit - counts[i], max(1, left * weights[i] // mass), spare)
            counts[i] = counts[i] + addition
            spare = spare - addition
    return np.array(counts)


def noise(rng, dims, width, limit, cuts=(), kind=jnp.bfloat16):
    values = jax.random.normal(rng, dims, jnp.float32) * width
    if len(cuts) > 0:
        values = steps_of(rng, dims, cuts, -0.22, 0.18) * values
    return jnp.clip(values, min=-limit, max=limit).astype(kind)


def heavy_noise(stream_key, dims, deviation, most, shards, heavy, kind=jnp.bfloat16):
    result = deviation * jax.random.normal(stream_key, dims, jnp.float32)
    if shards:
        result = result * steps_of(stream_key, dims, shards, -0.22, 0.18)
    return jnp.clip(strengthened(result, jax.random.fold_in(stream_key, 3), *heavy), -most, most).astype(kind)


def setup_inputs(seed: int = 0, part: int = 0) -> dict:
    splits = jax.random.split(jax.random.key(seed), 12)
    part_splits = jax.random.split(jax.random.fold_in(splits[11], part), 12)
    queries = draw_queries(jax.random.fold_in(jax.random.fold_in(splits[11], part), 71), part)
    key_cache = draw_key_cache(jax.random.fold_in(jax.random.fold_in(splits[11], part), 71), part)
    value_cache = noise(part_splits[2], (SEQS, CONTEXT, KVH * HD), 1.0, 6.0, ((1, 32),))
    out_weight = heavy_noise(splits[3], (HEADS * HD, D), (HEADS * HD) ** -0.5, 0.125, ((0, 32),), (0, 1, 32, 2.75))
    hidden_in = draw_hidden_in(jax.random.fold_in(jax.random.fold_in(splits[11], part), 71), part)
    norm_gain = jnp.clip(1.0 + 0.15 * jax.random.normal(splits[5], (D,), jnp.float32), 0.25, 1.75)
    gate_weight = noise(splits[6], (SHARDS, D, HID_DEV), D ** -0.5, 0.09375, ((0, 32),))
    up_weight = noise(splits[7], (SHARDS, D, HID_DEV), D ** -0.5, 0.09375, ((0, 32),))
    down_weight = noise(splits[8], (SHARDS, HID_DEV, D), FF ** -0.5, 0.15625, ((0, 32),))
    routes_keys = jax.random.split(jax.random.fold_in(part_splits[9], 1), SEQS // SEQS)
    routes_turns = jax.random.permutation(jax.random.fold_in(part_splits[9], 3), SEQS // SEQS)
    routes = jax.vmap(lambda own, number: shared_out(jax.random.fold_in(part_splits[9], 2), own, number, SEQS, EXPERTS, TOP, CAP, 2))(routes_keys, routes_turns).reshape((SEQS, TOP))
    route_weight = jnp.clip(jax.random.uniform(part_splits[10], (SEQS, TOP), jnp.float32, 0.1, 1.0), 0.1, 1.0)
    return {"queries": queries, "key_cache": key_cache, "value_cache": value_cache, "out_weight": out_weight, "hidden_in": hidden_in, "norm_gain": norm_gain, "gate_weight": gate_weight, "up_weight": up_weight, "down_weight": down_weight, "routes": routes, "route_weight": route_weight}


def slot_numbers(routes, expert_count):
    flat_routes = routes.reshape(-1)
    onehot = (flat_routes[:, None] == jnp.arange(expert_count, dtype=jnp.int32)[None, :]).astype(jnp.int32)
    before = jnp.cumsum(onehot, axis=0) - onehot
    return lax.optimization_barrier(jnp.sum(before * onehot, axis=1)).astype(jnp.int32)

def reference(queries, key_cache, value_cache, out_weight, hidden_in, norm_gain, gate_weight, up_weight, down_weight, routes, route_weight):
    group_size = HEADS // KVH
    query_view = queries.reshape(SEQS, KVH, group_size, HD).astype(jnp.float32)
    key_view = key_cache.reshape(SEQS, CONTEXT, KVH, HD).astype(jnp.float32)
    value_view = value_cache.reshape(SEQS, CONTEXT, KVH, HD).astype(jnp.float32)
    scores = jnp.einsum('sgjd,scgd->sgjc', query_view, key_view) * HD ** (-0.5)
    row_peak = lax.optimization_barrier(jnp.max(scores, axis=-1, keepdims=True))
    numer = jnp.exp(scores - row_peak)
    denoms = lax.optimization_barrier(jnp.sum(numer, axis=-1))
    probs = lax.optimization_barrier(numer.astype(jnp.bfloat16)).astype(jnp.float32)
    weighted = jnp.einsum('sgjc,scgd->sgjd', probs, value_view)
    attended = (weighted / denoms[..., None]).reshape(SEQS, HEADS * HD).astype(jnp.bfloat16)
    projected = jnp.dot(attended, out_weight, preferred_element_type=jnp.float32)
    resid = hidden_in.astype(jnp.float32) + projected
    inverse_rms = lax.rsqrt(lax.optimization_barrier(jnp.mean(resid * resid, axis=-1, keepdims=True)) + 1e-06)
    normed = (resid * inverse_rms * norm_gain.astype(jnp.float32)).astype(jnp.bfloat16)
    slot_index = slot_numbers(routes, EXPERTS)
    flat_routes = routes.reshape(-1)
    token_of = jnp.arange(SEQS * TOP, dtype=jnp.int32) // TOP
    weight_flat = route_weight.reshape(-1).astype(jnp.float32)
    slot_range = jnp.arange(CAP, dtype=jnp.int32)

    def one_shard(shard_args):
        shard_index, gate_part, up_part, down_part = shard_args
        expert = shard_index // QUARTERS
        matches = (flat_routes[None, :] == expert) & (slot_index[None, :] == slot_range[:, None])
        slot_token = lax.optimization_barrier(jnp.sum(matches.astype(jnp.int32) * token_of[None, :], axis=1)).astype(jnp.int32)
        slot_weight = lax.optimization_barrier(jnp.sum(matches.astype(jnp.float32) * weight_flat[None, :], axis=1))
        picked_rows = normed[slot_token]
        gate_act = jnp.dot(picked_rows, gate_part, preferred_element_type=jnp.float32)
        up_act = jnp.dot(picked_rows, up_part, preferred_element_type=jnp.float32)
        hidden = (jax.nn.silu(gate_act) * up_act).astype(jnp.bfloat16)
        return jnp.dot(hidden, down_part, preferred_element_type=jnp.float32) * slot_weight[:, None]
    expert_out = lax.map(one_shard, (jnp.arange(SHARDS, dtype=jnp.int32), gate_weight, up_weight, down_weight))
    grouped = expert_out.reshape(EXPERTS, QUARTERS, CAP, D)
    gathered = grouped[routes, :, slot_index.reshape(SEQS, TOP)]
    moe = lax.optimization_barrier(jnp.sum(gathered, axis=(1, 2)))
    return resid + moe
```

```python
import jax
import jax.numpy as jnp
from jax import lax
from jax.sharding import PartitionSpec as P

QUARTERS = 8


eps = 1e-06


def swap_blocks(blocks):
    return lax.all_to_all(blocks, "ctx", split_axis=0, concat_axis=0, tiled=True)


def body(
    queries,
    key_cache,
    value_cache,
    out_weight,
    hidden_in,
    norm_gain,
    gate_weight,
    up_weight,
    down_weight,
    routes,
    route_weight,
):
    devices = lax.axis_size("ctx")
    my_index = lax.axis_index("ctx")
    seq_count, head_count, head_dim = queries.shape
    kv_heads = key_cache.shape[2] // head_dim
    group_size = head_count // kv_heads
    model_width = hidden_in.shape[1]
    local_len = key_cache.shape[1]
    query_view = queries.reshape(seq_count, kv_heads, group_size, head_dim)
    key_view = key_cache.reshape(seq_count, local_len, kv_heads, head_dim)
    value_view = value_cache.reshape(seq_count, local_len, kv_heads, head_dim)
    scores = jnp.einsum(
        "sgjd,scgd->sgjc", query_view, key_view, preferred_element_type=jnp.float32
    ) * head_dim ** (-0.5)
    peak = jnp.max(scores, axis=-1)
    numer = jnp.exp(scores - peak[..., None])
    denom = jnp.sum(numer, axis=-1)
    weighted = jnp.einsum(
        "sgjc,scgd->sgjd",
        numer.astype(jnp.bfloat16),
        value_view,
        preferred_element_type=jnp.float32,
    )
    feat_dev = head_count * head_dim // devices
    spread = max(1, head_dim // feat_dev)
    heads_dev = max(1, feat_dev // head_dim)
    width = feat_dev // heads_dev

    def by_owner(stat):
        stat = jnp.repeat(stat.reshape(seq_count, head_count), spread, axis=1)
        return stat.reshape(seq_count, devices, heads_dev).transpose(1, 0, 2)

    weighted = weighted.reshape(seq_count, devices, heads_dev, width).transpose(1, 0, 2, 3)
    stats = jnp.stack([by_owner(peak), by_owner(denom)], axis=-1)
    sent = jnp.concatenate(
        [weighted.reshape(devices, -1), stats.reshape(devices, -1)], axis=1
    )
    got = swap_blocks(sent)
    parts = got[:, : seq_count * feat_dev].reshape(devices, seq_count, heads_dev, width)
    stats = got[:, seq_count * feat_dev :].reshape(devices, seq_count, heads_dev, 2)
    peaks = stats[..., 0]
    scale = jnp.exp(peaks - jnp.max(peaks, axis=0))
    denoms = jnp.sum(scale * stats[..., 1], axis=0)
    summed = jnp.sum(scale[..., None] * parts, axis=0)
    attended = (summed / denoms[..., None]).reshape(seq_count, feat_dev).astype(jnp.bfloat16)
    proj_part = jnp.dot(attended, out_weight, preferred_element_type=jnp.float32)
    col_dev = model_width // devices
    col_start = my_index * col_dev

    def to_owner(rows):
        blocks = rows.reshape(seq_count, devices, col_dev).transpose(1, 0, 2)
        return jnp.sum(swap_blocks(blocks).astype(jnp.float32), axis=0)

    hidden_mine = lax.dynamic_slice_in_dim(hidden_in, col_start, col_dev, 1)
    resid_mine = hidden_mine.astype(jnp.float32) + to_owner(proj_part)
    resid = swap_blocks(jnp.broadcast_to(resid_mine, (devices, seq_count, col_dev)))
    resid = resid.transpose(1, 0, 2).reshape(seq_count, model_width)
    inverse_rms = lax.rsqrt(jnp.mean(resid * resid, axis=-1, keepdims=True) + eps)
    normed = (resid * inverse_rms * norm_gain).astype(jnp.bfloat16)
    expert = my_index // QUARTERS
    token_weight = jnp.sum(jnp.where(routes == expert, route_weight, 0.0), axis=1)
    gate_act = jnp.dot(normed, gate_weight[0], preferred_element_type=jnp.float32)
    up_act = jnp.dot(normed, up_weight[0], preferred_element_type=jnp.float32)
    hidden = (jax.nn.silu(gate_act) * up_act).astype(jnp.bfloat16)
    expert_out = (
        jnp.dot(hidden, down_weight[0], preferred_element_type=jnp.float32)
        * token_weight[:, None]
    )
    return resid_mine + to_owner(expert_out.astype(jnp.bfloat16))


def solution(mesh):
    in_specs = (
        P("group", None, None),
        P("group", "ctx", None),
        P("group", "ctx", None),
        P("ctx", None),
        P("group", None),
        P(),
        P("ctx", None, None),
        P("ctx", None, None),
        P("ctx", None, None),
        P("group", None),
        P("group", None),
    )
    out_specs = P("group", "ctx")
    return jax.shard_map(body, mesh=mesh, in_specs=in_specs, out_specs=out_specs, check_vma=False)
```

```python
import functools

import jax
import jax.numpy as jnp
from jax import lax
from jax.experimental import pallas as pl
from jax.experimental.pallas import tpu as pltpu
from jax.sharding import PartitionSpec as P

QUARTERS = 8


eps = 1e-06
LIMIT = 16 << 20
LONG = 1 << 34
f32 = jnp.float32
bf16 = jnp.bfloat16


def in_vmem(array):
    return pltpu.with_memory_space_constraint(array, pltpu.VMEM)


def in_hbm(array):
    return pltpu.with_memory_space_constraint(array, pltpu.HBM)


def call(kernel, out_shape, in_specs=None, count=0, scratch=(), flops=1 << 10, moved=1 << 10):
    vmem = pl.BlockSpec(memory_space=pltpu.VMEM)
    many = isinstance(out_shape, (tuple, list))
    return pl.pallas_call(
        kernel,
        out_shape=out_shape,
        in_specs=in_specs or [vmem] * count,
        out_specs=[vmem] * len(out_shape) if many else vmem,
        scratch_shapes=list(scratch),
        compiler_params=pltpu.CompilerParams(vmem_limit_bytes=LIMIT),
        cost_estimate=pl.CostEstimate(flops=flops, bytes_accessed=moved, transcendentals=0),
    )


def dot_nt(a, b):
    return lax.dot_general(a, b, (((1,), (1,)), ((), ())), preferred_element_type=f32)


def attend_kernel(heads_dev, kv_heads, q_hbm, k_hbm, v_hbm, out_ref, q, k, v, sems):
    seq_count, local_len, _ = k.shape
    head_dim = q.shape[1]
    head_count = q.shape[0] // seq_count
    copies = [
        pltpu.make_async_copy(src, dst, sems.at[n])
        for n, (src, dst) in enumerate(((q_hbm, q), (k_hbm, k), (v_hbm, v)))
    ]
    for copy in copies:
        copy.start()
    half = seq_count * heads_dev
    owners = head_count // kv_heads // heads_dev
    rows = owners * 2 * half
    row = lax.broadcasted_iota(jnp.int32, (rows, 1), 0)
    within = lax.rem(row, half)
    seq_of = lax.rem(within, seq_count)
    head_of = lax.div(row, 2 * half) * heads_dev + lax.div(within, seq_count)
    source = seq_of * head_count + head_of
    column = lax.broadcasted_iota(jnp.int32, (rows, q.shape[0]), 1)
    is_part = lax.rem(row, 2 * half) < half
    lane = lax.broadcasted_iota(jnp.int32, (rows, head_dim), 1)
    copies[0].wait()
    copies[1].wait()
    numers = []
    stats = []
    for g in range(kv_heads):
        pick = jnp.where(column == source + g * owners * heads_dev, 1.0, 0.0).astype(bf16)
        picked = jnp.dot(pick, q[...], preferred_element_type=f32).astype(bf16)
        feats = slice(g * head_dim, (g + 1) * head_dim)
        scores = dot_nt(picked, k[0, :, feats])
        for s in range(1, seq_count):
            scores = jnp.where(seq_of == s, dot_nt(picked, k[s, :, feats]), scores)
        scores = scores * head_dim ** (-0.5)
        peak = jnp.max(scores, axis=1, keepdims=True)
        numer = jnp.exp(scores - peak)
        denom = jnp.sum(numer, axis=1, keepdims=True)
        numers.append(numer.astype(bf16))
        stats.append(jnp.where(lane < head_dim // 2, peak, denom))
    copies[2].wait()
    for g in range(kv_heads):
        feats = slice(g * head_dim, (g + 1) * head_dim)
        part = jnp.dot(numers[g], v[0, :, feats], preferred_element_type=f32)
        for s in range(1, seq_count):
            other = jnp.dot(numers[g], v[s, :, feats], preferred_element_type=f32)
            part = jnp.where(seq_of == s, other, part)
        block = jnp.where(is_part, part, stats[g])
        out_ref[g * owners : (g + 1) * owners] = block.reshape(owners, 2 * half, head_dim)


def attend(queries, key_cache, value_cache, devices, heads_dev):
    seq_count, head_count, head_dim = queries.shape
    hbm = pl.BlockSpec(memory_space=pltpu.HBM)
    q = in_hbm(queries.reshape(seq_count * head_count, head_dim))
    kernel = functools.partial(attend_kernel, heads_dev, key_cache.shape[2] // head_dim)
    return call(
        kernel,
        jax.ShapeDtypeStruct((devices, 2 * seq_count * heads_dev, head_dim), f32),
        in_specs=[hbm] * 3,
        scratch=(
            pltpu.VMEM(q.shape, bf16),
            pltpu.VMEM(key_cache.shape, bf16),
            pltpu.VMEM(value_cache.shape, bf16),
            pltpu.SemaphoreType.DMA((3,)),
        ),
        flops=LONG,
    )(q, in_hbm(key_cache), in_hbm(value_cache))


def project_kernel(seq_count, got_ref, weight_ref, send_ref, keep_ref):
    core = lax.rem(lax.axis_index("ctx"), 2)
    head_dim = got_ref.shape[2]
    half = got_ref.shape[1] // 2
    stats = got_ref[:, half:, :]
    peaks = stats[:, :, 0:1]
    scale = jnp.exp(peaks - jnp.max(peaks, axis=0, keepdims=True))
    denoms = jnp.sum(scale * stats[:, :, head_dim // 2 : head_dim // 2 + 1], axis=0)
    summed = jnp.sum(scale * got_ref[:, :half, :], axis=0)
    attended = (summed / denoms).astype(bf16)
    attended = jnp.concatenate(
        [attended[n : n + seq_count] for n in range(0, half, seq_count)], axis=1
    )
    mid = weight_ref.shape[1] // 2
    low = jnp.dot(attended, weight_ref[:, :mid], preferred_element_type=f32)
    high = jnp.dot(attended, weight_ref[:, mid:], preferred_element_type=f32)
    send_ref[...] = jnp.where(core == 0, high, low)
    keep_ref[...] = jnp.where(core == 0, low, high)


def spread_kernel(keep_ref, came_ref, out_ref):
    total = (keep_ref[...] + came_ref[...]).astype(out_ref.dtype)
    for n in range(out_ref.shape[0]):
        out_ref[n] = total


def resid_kernel(got_ref, hidden_ref, out_ref):
    core = lax.rem(lax.axis_index("ctx"), 2)
    mid = out_ref.shape[1]
    hidden = jnp.where(core == 0, hidden_ref[:, :mid].astype(f32), hidden_ref[:, mid:].astype(f32))
    total = got_ref[0].astype(f32)
    for n in range(1, got_ref.shape[0]):
        total = total + got_ref[n].astype(f32)
    out_ref[...] = hidden + total


def expert_kernel(
    mine_ref, came_ref, gain_ref, gate_ref, up_ref, down_ref, routes_ref, share_ref, out_ref, mine_out, resid_ref
):
    index = lax.axis_index("ctx")
    core = lax.rem(index, 2)
    expert = lax.div(index, QUARTERS)
    mid = mine_ref.shape[1]
    low = jnp.where(core == 0, mine_ref[...], came_ref[...])
    high = jnp.where(core == 0, came_ref[...], mine_ref[...])
    resid_ref[:, :mid] = low
    resid_ref[:, mid:] = high
    col_dev = mine_out.shape[1]
    if col_dev == 2 * mid:
        mine_out[...] = resid_ref[...]
    else:
        start = pl.multiple_of(index * col_dev, col_dev)
        mine_out[...] = resid_ref[:, pl.ds(start, col_dev)]
    square = jnp.sum(low * low, axis=1, keepdims=True) + jnp.sum(high * high, axis=1, keepdims=True)
    inverse_rms = lax.rsqrt(square / (2 * mid) + eps)
    low = (low * inverse_rms * gain_ref[:, :mid]).astype(bf16)
    high = (high * inverse_rms * gain_ref[:, mid:]).astype(bf16)
    gate_act = dot_nt(low, gate_ref[:, :mid]) + dot_nt(high, gate_ref[:, mid:])
    up_act = dot_nt(low, up_ref[:, :mid]) + dot_nt(high, up_ref[:, mid:])
    hidden = (gate_act / (1.0 + jnp.exp(-gate_act)) * up_act).astype(bf16)
    share = jnp.where(routes_ref[...] == expert, share_ref[...], 0.0)
    share = jnp.sum(share, axis=1, keepdims=True)
    out = jnp.dot(hidden, down_ref[...], preferred_element_type=f32)
    out_ref[...] = (out * share).astype(bf16)


def merge_parts(queries, key_cache, value_cache, devices):
    seq_count, head_count, head_dim = queries.shape
    kv_heads = key_cache.shape[2] // head_dim
    local_len = key_cache.shape[1]
    query_view = queries.reshape(seq_count, kv_heads, head_count // kv_heads, head_dim)
    key_view = key_cache.reshape(seq_count, local_len, kv_heads, head_dim)
    value_view = value_cache.reshape(seq_count, local_len, kv_heads, head_dim)
    scores = jnp.einsum(
        "sgjd,scgd->sgjc", query_view, key_view, preferred_element_type=f32
    ) * head_dim ** (-0.5)
    peak = jnp.max(scores, axis=-1)
    numer = jnp.exp(scores - peak[..., None])
    denom = jnp.sum(numer, axis=-1)
    weighted = jnp.einsum(
        "sgjc,scgd->sgjd", numer.astype(bf16), value_view, preferred_element_type=f32
    )
    width = head_count * head_dim // devices
    spread = head_dim // width

    def by_owner(stat):
        return jnp.repeat(stat.reshape(seq_count, head_count), spread, axis=1).T[..., None]

    weighted = weighted.reshape(seq_count, devices, width).transpose(1, 0, 2)
    sent = jnp.concatenate([weighted, by_owner(peak), by_owner(denom)], axis=2)
    got = swap_blocks(sent)
    peaks = got[:, :, width : width + 1]
    scale = jnp.exp(peaks - jnp.max(peaks, axis=0))
    denoms = jnp.sum(scale * got[:, :, width + 1 :], axis=0)
    return (jnp.sum(scale * got[:, :, :width], axis=0) / denoms).astype(bf16)


def swap_blocks(blocks, groups=None):
    return lax.all_to_all(
        blocks, "ctx", split_axis=0, concat_axis=0, tiled=True, axis_index_groups=groups
    )


def body(
    queries,
    key_cache,
    value_cache,
    out_weight,
    hidden_in,
    norm_gain,
    gate_weight,
    up_weight,
    down_weight,
    routes,
    route_weight,
):
    devices = lax.axis_size("ctx")
    my_index = lax.axis_index("ctx")
    seq_count, head_count, head_dim = queries.shape
    model_width = hidden_in.shape[1]
    mid = model_width // 2
    feat_dev = head_count * head_dim // devices
    half = jax.ShapeDtypeStruct((seq_count, mid), f32)
    if feat_dev % head_dim == 0:
        heads_dev = feat_dev // head_dim
        got = swap_blocks(attend(queries, key_cache, value_cache, devices, heads_dev))
        send, keep = call(functools.partial(project_kernel, seq_count), (half, half), count=2)(
            got, in_vmem(out_weight)
        )
    else:
        attended = merge_parts(queries, key_cache, value_cache, devices)
        proj = jnp.dot(attended, out_weight, preferred_element_type=f32)
        low, high = proj[:, :mid], proj[:, mid:]
        first = lax.rem(my_index, 2) == 0
        send, keep = jnp.where(first, high, low), jnp.where(first, low, high)
    pairs = [(n, n ^ 1) for n in range(devices)]
    chips = devices // 2
    groups = [[2 * n + core for n in range(chips)] for core in range(2)]
    came = lax.ppermute(send, "ctx", pairs)
    spread = call(spread_kernel, jax.ShapeDtypeStruct((chips, seq_count, mid), bf16), count=2, flops=LONG)(
        keep, came
    )
    mine = call(resid_kernel, half, count=2)(swap_blocks(spread, groups), hidden_in)
    came = lax.ppermute(mine, "ctx", pairs)
    col_dev = model_width // devices
    aligned = col_dev % 128 == 0
    out, resid_mine = call(
        expert_kernel,
        (
            jax.ShapeDtypeStruct((seq_count, model_width), bf16),
            jax.ShapeDtypeStruct((seq_count, col_dev if aligned else model_width), f32),
        ),
        count=8,
        scratch=(pltpu.VMEM((seq_count, model_width), f32),),
    )(
        mine,
        came,
        norm_gain.reshape(1, model_width),
        in_vmem(gate_weight[0].T),
        in_vmem(up_weight[0].T),
        in_vmem(down_weight[0]),
        routes,
        route_weight,
    )
    blocks = lax.all_to_all(
        out.reshape(seq_count, devices, col_dev), "ctx", split_axis=1, concat_axis=1, tiled=True
    )
    if not aligned:
        resid_mine = lax.dynamic_slice_in_dim(resid_mine, my_index * col_dev, col_dev, 1)
    return resid_mine + jnp.sum(blocks.astype(f32), axis=1)


def solution(mesh):
    in_specs = (
        P("group", None, None),
        P("group", "ctx", None),
        P("group", "ctx", None),
        P("ctx", None),
        P("group", None),
        P(),
        P("ctx", None, None),
        P("ctx", None, None),
        P("ctx", None, None),
        P("group", None),
        P("group", None),
    )
    out_specs = P("group", "ctx")
    return jax.shard_map(body, mesh=mesh, in_specs=in_specs, out_specs=out_specs, check_vma=False)
```

```python
import functools

import jax
import jax.numpy as jnp
from jax import lax
from jax.experimental import pallas as pl
from jax.experimental.pallas import tpu as pltpu
from jax.sharding import PartitionSpec as P

QUARTERS = 8


eps = 1e-06
LIMIT = 16 << 20
LONG = 1 << 34
f32 = jnp.float32
bf16 = jnp.bfloat16


def in_vmem(array):
    return pltpu.with_memory_space_constraint(array, pltpu.VMEM)


def in_hbm(array):
    return pltpu.with_memory_space_constraint(array, pltpu.HBM)


def call(kernel, out_shape, in_specs=None, count=0, scratch=(), flops=1 << 10, moved=1 << 10):
    vmem = pl.BlockSpec(memory_space=pltpu.VMEM)
    many = isinstance(out_shape, (tuple, list))
    return pl.pallas_call(
        kernel,
        out_shape=out_shape,
        in_specs=in_specs or [vmem] * count,
        out_specs=[vmem] * len(out_shape) if many else vmem,
        scratch_shapes=list(scratch),
        compiler_params=pltpu.CompilerParams(vmem_limit_bytes=LIMIT),
        cost_estimate=pl.CostEstimate(flops=flops, bytes_accessed=moved, transcendentals=0),
    )


def dot_nt(a, b):
    return lax.dot_general(a, b, (((1,), (1,)), ((), ())), preferred_element_type=f32)


def attend_kernel(heads_dev, kv_heads, q_hbm, k_hbm, v_hbm, w_hbm, out_ref, w_ref, q, k, v, sems):
    seq_count, local_len, _ = k.shape
    head_dim = q.shape[1]
    head_count = q.shape[0] // seq_count
    moves = ((q_hbm, q), (k_hbm, k), (v_hbm, v), (w_hbm, w_ref))
    copies = [pltpu.make_async_copy(src, dst, sems.at[n]) for n, (src, dst) in enumerate(moves)]
    for copy in copies:
        copy.start()
    half = seq_count * heads_dev
    owners = head_count // kv_heads // heads_dev
    rows = owners * 2 * half
    row = lax.broadcasted_iota(jnp.int32, (rows, 1), 0)
    within = lax.rem(row, half)
    seq_of = lax.rem(within, seq_count)
    head_of = lax.div(row, 2 * half) * heads_dev + lax.div(within, seq_count)
    source = seq_of * head_count + head_of
    column = lax.broadcasted_iota(jnp.int32, (rows, q.shape[0]), 1)
    picks = [
        jnp.where(column == source + g * owners * heads_dev, 1.0, 0.0).astype(bf16)
        for g in range(kv_heads)
    ]
    is_part = lax.rem(row, 2 * half) < half
    lane = lax.broadcasted_iota(jnp.int32, (rows, head_dim), 1)
    third = head_dim // 3

    def by_seq(values):
        return jnp.concatenate(
            [jnp.where(seq_of == s, values, 0.0).astype(bf16) for s in range(seq_count)], axis=1
        )

    copies[0].wait()
    queries = [by_seq(jnp.dot(pick, q[...], preferred_element_type=f32)) for pick in picks]
    copies[1].wait()
    feats = [slice(g * head_dim, (g + 1) * head_dim) for g in range(kv_heads)]
    scores = [
        dot_nt(queries[g], jnp.concatenate([k[s, :, feats[g]] for s in range(seq_count)], axis=1))
        * head_dim ** (-0.5)
        for g in range(kv_heads)
    ]
    numers = []
    stats = []
    for g in range(kv_heads):
        peak = jnp.max(scores[g], axis=1, keepdims=True).astype(bf16).astype(f32)
        numer = jnp.exp(scores[g] - peak)
        denom = jnp.sum(numer, axis=1, keepdims=True)
        coarse = denom.astype(bf16).astype(f32)
        totals = jnp.where(lane < 2 * third, coarse, denom - coarse)
        stats.append(jnp.where(lane < third, peak, totals))
        numers.append(by_seq(numer))
    copies[2].wait()
    for g in range(kv_heads):
        values = jnp.concatenate([v[s, :, feats[g]] for s in range(seq_count)], axis=0)
        part = jnp.dot(numers[g], values, preferred_element_type=f32)
        block = jnp.where(is_part, part, stats[g]).astype(bf16)
        out_ref[g * owners : (g + 1) * owners] = block.reshape(owners, 2 * half, head_dim)
    copies[3].wait()


def attend(queries, key_cache, value_cache, out_weight, devices, heads_dev):
    seq_count, head_count, head_dim = queries.shape
    hbm = pl.BlockSpec(memory_space=pltpu.HBM)
    q = queries.reshape(seq_count * head_count, head_dim)
    kernel = functools.partial(attend_kernel, heads_dev, key_cache.shape[2] // head_dim)
    return call(
        kernel,
        (
            pltpu.VMEM((devices, 2 * seq_count * heads_dev, head_dim), bf16),
            pltpu.VMEM(out_weight.shape, bf16),
        ),
        in_specs=[hbm] * 4,
        scratch=(
            pltpu.VMEM(q.shape, bf16),
            pltpu.VMEM(key_cache.shape, bf16),
            pltpu.VMEM(value_cache.shape, bf16),
            pltpu.SemaphoreType.DMA((4,)),
        ),
    )(in_hbm(q), in_hbm(key_cache), in_hbm(value_cache), in_hbm(out_weight))


def project_kernel(seq_count, got_ref, weight_ref, send_ref, keep_ref):
    core = lax.rem(lax.axis_index("ctx"), 2)
    head_dim = got_ref.shape[2]
    half = got_ref.shape[1] // 2
    got = got_ref[...].astype(f32)
    third = head_dim // 3
    stats = got[:, half:, :]
    peaks = stats[:, :, 0:1]
    scale = jnp.exp(peaks - jnp.max(peaks, axis=0, keepdims=True))
    total = stats[:, :, third : third + 1] + stats[:, :, 2 * third : 2 * third + 1]
    denoms = jnp.sum(scale * total, axis=0)
    summed = jnp.sum(scale * got[:, :half, :], axis=0)
    attended = (summed / denoms).astype(bf16)
    attended = jnp.concatenate(
        [attended[n : n + seq_count] for n in range(0, half, seq_count)], axis=1
    )
    mid = weight_ref.shape[1] // 2
    low = jnp.dot(attended, weight_ref[:, :mid], preferred_element_type=f32)
    high = jnp.dot(attended, weight_ref[:, mid:], preferred_element_type=f32)
    send_ref[...] = jnp.where(core == 0, high, low)
    keep_ref[...] = jnp.where(core == 0, low, high)


def spread_kernel(keep_ref, came_ref, out_ref):
    total = (keep_ref[...] + came_ref[...]).astype(out_ref.dtype)
    quarter = out_ref.shape[2]
    for n in range(out_ref.shape[0]):
        out_ref[n] = total[:, n % 2 * quarter : (n % 2 + 1) * quarter]


def resid_kernel(got_ref, hidden_ref, out_ref):
    core = lax.rem(lax.axis_index("ctx"), 2)
    quarter = got_ref.shape[2]
    for side in range(2):
        start = 2 * side * quarter
        hidden = jnp.where(
            core == 0,
            hidden_ref[:, start : start + quarter].astype(f32),
            hidden_ref[:, start + quarter : start + 2 * quarter].astype(f32),
        )
        total = got_ref[side].astype(f32)
        for n in range(side + 2, got_ref.shape[0], 2):
            total = total + got_ref[n].astype(f32)
        out_ref[:, side * quarter : (side + 1) * quarter] = hidden + total


def expert_kernel(
    mine_ref, came_ref, gain_ref, gate_ref, up_ref, down_ref, routes_ref, share_ref, out_ref, mine_out, resid_ref
):
    index = lax.axis_index("ctx")
    core = lax.rem(index, 2)
    expert = lax.div(index, QUARTERS)
    mid = mine_ref.shape[1]
    even = jnp.where(core == 0, mine_ref[...], came_ref[...])
    odd = jnp.where(core == 0, came_ref[...], mine_ref[...])
    low = jnp.concatenate([even[:, : mid // 2], odd[:, : mid // 2]], axis=1)
    high = jnp.concatenate([even[:, mid // 2 :], odd[:, mid // 2 :]], axis=1)
    resid_ref[:, :mid] = low
    resid_ref[:, mid:] = high
    col_dev = mine_out.shape[1]
    if col_dev == 2 * mid:
        mine_out[...] = resid_ref[...]
    else:
        start = pl.multiple_of(index * col_dev, col_dev)
        mine_out[...] = resid_ref[:, pl.ds(start, col_dev)]
    square = jnp.sum(low * low, axis=1, keepdims=True) + jnp.sum(high * high, axis=1, keepdims=True)
    inverse_rms = lax.rsqrt(square / (2 * mid) + eps)
    low = (low * inverse_rms * gain_ref[:, :mid]).astype(bf16)
    high = (high * inverse_rms * gain_ref[:, mid:]).astype(bf16)
    gate_act = dot_nt(low, gate_ref[:, :mid]) + dot_nt(high, gate_ref[:, mid:])
    up_act = dot_nt(low, up_ref[:, :mid]) + dot_nt(high, up_ref[:, mid:])
    hidden = (gate_act / (1.0 + jnp.exp(-gate_act)) * up_act).astype(bf16)
    share = jnp.where(routes_ref[...] == expert, share_ref[...], 0.0)
    share = jnp.sum(share, axis=1, keepdims=True)
    out = jnp.dot(hidden, down_ref[...], preferred_element_type=f32)
    out_ref[...] = (out * share).astype(bf16)


def merge_parts(queries, key_cache, value_cache, devices):
    seq_count, head_count, head_dim = queries.shape
    kv_heads = key_cache.shape[2] // head_dim
    local_len = key_cache.shape[1]
    query_view = queries.reshape(seq_count, kv_heads, head_count // kv_heads, head_dim)
    key_view = key_cache.reshape(seq_count, local_len, kv_heads, head_dim)
    value_view = value_cache.reshape(seq_count, local_len, kv_heads, head_dim)
    scores = jnp.einsum(
        "sgjd,scgd->sgjc", query_view, key_view, preferred_element_type=f32
    ) * head_dim ** (-0.5)
    peak = jnp.max(scores, axis=-1)
    numer = jnp.exp(scores - peak[..., None])
    denom = jnp.sum(numer, axis=-1)
    weighted = jnp.einsum(
        "sgjc,scgd->sgjd", numer.astype(bf16), value_view, preferred_element_type=f32
    )
    width = head_count * head_dim // devices
    spread = head_dim // width

    def by_owner(stat):
        return jnp.repeat(stat.reshape(seq_count, head_count), spread, axis=1).T[..., None]

    weighted = weighted.reshape(seq_count, devices, width).transpose(1, 0, 2)
    sent = jnp.concatenate([weighted, by_owner(peak), by_owner(denom)], axis=2)
    got = swap_blocks(sent)
    peaks = got[:, :, width : width + 1]
    scale = jnp.exp(peaks - jnp.max(peaks, axis=0))
    denoms = jnp.sum(scale * got[:, :, width + 1 :], axis=0)
    return (jnp.sum(scale * got[:, :, :width], axis=0) / denoms).astype(bf16)


def swap_blocks(blocks):
    return lax.all_to_all(blocks, "ctx", split_axis=0, concat_axis=0, tiled=True)


def body(
    queries,
    key_cache,
    value_cache,
    out_weight,
    hidden_in,
    norm_gain,
    gate_weight,
    up_weight,
    down_weight,
    routes,
    route_weight,
):
    devices = lax.axis_size("ctx")
    my_index = lax.axis_index("ctx")
    seq_count, head_count, head_dim = queries.shape
    model_width = hidden_in.shape[1]
    mid = model_width // 2
    feat_dev = head_count * head_dim // devices
    half = jax.ShapeDtypeStruct((seq_count, mid), f32)
    if feat_dev % head_dim == 0:
        heads_dev = feat_dev // head_dim
        parts, weight = attend(queries, key_cache, value_cache, out_weight, devices, heads_dev)
        send, keep = call(functools.partial(project_kernel, seq_count), (half, half), count=2)(
            swap_blocks(parts), weight
        )
    else:
        attended = merge_parts(queries, key_cache, value_cache, devices)
        proj = jnp.dot(attended, out_weight, preferred_element_type=f32)
        low, high = proj[:, :mid], proj[:, mid:]
        first = lax.rem(my_index, 2) == 0
        send, keep = jnp.where(first, high, low), jnp.where(first, low, high)
    pairs = [(n, n ^ 1) for n in range(devices)]
    came = lax.ppermute(send, "ctx", pairs)
    spread = call(
        spread_kernel,
        jax.ShapeDtypeStruct((devices, seq_count, mid // 2), bf16),
        count=2,
        flops=LONG,
    )(keep, came)
    mine = call(resid_kernel, half, count=2)(swap_blocks(spread), hidden_in)
    came = lax.ppermute(mine, "ctx", pairs)
    col_dev = model_width // devices
    aligned = col_dev % 128 == 0
    out, resid_mine = call(
        expert_kernel,
        (
            jax.ShapeDtypeStruct((seq_count, model_width), bf16),
            jax.ShapeDtypeStruct((seq_count, col_dev if aligned else model_width), f32),
        ),
        count=8,
        scratch=(pltpu.VMEM((seq_count, model_width), f32),),
    )(
        mine,
        came,
        norm_gain.reshape(1, model_width),
        in_vmem(gate_weight[0].T),
        in_vmem(up_weight[0].T),
        in_vmem(down_weight[0]),
        routes,
        route_weight,
    )
    blocks = lax.all_to_all(
        out.reshape(seq_count, devices, col_dev), "ctx", split_axis=1, concat_axis=1, tiled=True
    )
    if not aligned:
        resid_mine = lax.dynamic_slice_in_dim(resid_mine, my_index * col_dev, col_dev, 1)
    return resid_mine + jnp.sum(blocks.astype(f32), axis=1)


def solution(mesh):
    in_specs = (
        P("group", None, None),
        P("group", "ctx", None),
        P("group", "ctx", None),
        P("ctx", None),
        P("group", None),
        P(),
        P("ctx", None, None),
        P("ctx", None, None),
        P("ctx", None, None),
        P("group", None),
        P("group", None),
    )
    out_specs = P("group", "ctx")
    return jax.shard_map(body, mesh=mesh, in_specs=in_specs, out_specs=out_specs, check_vma=False)
```

```python
import functools

import jax
import jax.numpy as jnp
from jax import lax
from jax.experimental import pallas as pl
from jax.experimental.pallas import tpu as pltpu
from jax.sharding import PartitionSpec as P

QUARTERS = 8


eps = 1e-06
LIMIT = 16 << 20
LONG = 1 << 34
f32 = jnp.float32
bf16 = jnp.bfloat16


def in_vmem(array):
    return pltpu.with_memory_space_constraint(array, pltpu.VMEM)


def in_hbm(array):
    return pltpu.with_memory_space_constraint(array, pltpu.HBM)


def call(kernel, out_shape, in_specs=None, count=0, scratch=(), flops=1 << 10, moved=1 << 10):
    vmem = pl.BlockSpec(memory_space=pltpu.VMEM)
    many = isinstance(out_shape, (tuple, list))
    return pl.pallas_call(
        kernel,
        out_shape=out_shape,
        in_specs=in_specs or [vmem] * count,
        out_specs=[vmem] * len(out_shape) if many else vmem,
        scratch_shapes=list(scratch),
        compiler_params=pltpu.CompilerParams(vmem_limit_bytes=LIMIT),
        cost_estimate=pl.CostEstimate(flops=flops, bytes_accessed=moved, transcendentals=0),
    )


def dot_nt(a, b):
    return lax.dot_general(a, b, (((1,), (1,)), ((), ())), preferred_element_type=f32)


def attend_kernel(heads_dev, kv_heads, q_hbm, k_hbm, v_hbm, out_ref, q, k, v, sems):
    seq_count, local_len, _ = k.shape
    head_dim = q.shape[1]
    head_count = q.shape[0] // seq_count
    moves = ((k_hbm, k), (q_hbm, q), (v_hbm, v))
    copies = [pltpu.make_async_copy(src, dst, sems.at[n]) for n, (src, dst) in enumerate(moves)]
    for copy in copies:
        copy.start()
    half = seq_count * heads_dev
    owners = head_count // kv_heads // heads_dev
    rows = owners * 2 * half
    row = lax.broadcasted_iota(jnp.int32, (rows, 1), 0)
    within = lax.rem(row, half)
    seq_of = lax.rem(within, seq_count)
    head_of = lax.div(row, 2 * half) * heads_dev + lax.div(within, seq_count)
    source = seq_of * head_count + head_of
    column = lax.broadcasted_iota(jnp.int32, (rows, q.shape[0]), 1)
    picks = [
        jnp.where(column == source + g * owners * heads_dev, 1.0, 0.0).astype(bf16)
        for g in range(kv_heads)
    ]
    is_part = lax.rem(row, 2 * half) < half
    lane = lax.broadcasted_iota(jnp.int32, (rows, head_dim), 1)
    third = head_dim // 3

    def by_seq(values):
        return jnp.concatenate(
            [jnp.where(seq_of == s, values, 0.0).astype(bf16) for s in range(seq_count)], axis=1
        )

    copies[1].wait()
    queries = [by_seq(jnp.dot(pick, q[...], preferred_element_type=f32)) for pick in picks]
    copies[0].wait()
    copies[2].wait()
    feats = [slice(g * head_dim, (g + 1) * head_dim) for g in range(kv_heads)]
    scores = [
        dot_nt(queries[g], jnp.concatenate([k[s, :, feats[g]] for s in range(seq_count)], axis=1))
        * head_dim ** (-0.5)
        for g in range(kv_heads)
    ]
    numers = []
    stats = []
    for g in range(kv_heads):
        peak = jnp.max(scores[g], axis=1, keepdims=True).astype(bf16).astype(f32)
        numer = jnp.exp(scores[g] - peak)
        denom = jnp.sum(numer, axis=1, keepdims=True)
        coarse = denom.astype(bf16).astype(f32)
        totals = jnp.where(lane < 2 * third, coarse, denom - coarse)
        stats.append(jnp.where(lane < third, peak, totals))
        numers.append(by_seq(numer))
    for g in range(kv_heads):
        values = jnp.concatenate([v[s, :, feats[g]] for s in range(seq_count)], axis=0)
        part = jnp.dot(numers[g], values, preferred_element_type=f32)
        block = jnp.where(is_part, part, stats[g]).astype(bf16)
        out_ref[g * owners : (g + 1) * owners] = block.reshape(owners, 2 * half, head_dim)


def attend(queries, key_cache, value_cache, devices, heads_dev):
    seq_count, head_count, head_dim = queries.shape
    hbm = pl.BlockSpec(memory_space=pltpu.HBM)
    q = queries.reshape(seq_count * head_count, head_dim)
    kernel = functools.partial(attend_kernel, heads_dev, key_cache.shape[2] // head_dim)
    return call(
        kernel,
        pltpu.VMEM((devices, 2 * seq_count * heads_dev, head_dim), bf16),
        in_specs=[hbm] * 3,
        scratch=(
            pltpu.VMEM(q.shape, bf16),
            pltpu.VMEM(key_cache.shape, bf16),
            pltpu.VMEM(value_cache.shape, bf16),
            pltpu.SemaphoreType.DMA((3,)),
        ),
        flops=LONG,
    )(in_hbm(q), in_hbm(key_cache), in_hbm(value_cache))


def columns(block, width):
    return pl.ds(pl.multiple_of(block * width, width), width)


def send_kernel(seq_count, got_ref, weight_ref, send_ref, attended_ref):
    core = lax.rem(lax.axis_index("ctx"), 2)
    head_dim = got_ref.shape[2]
    half = got_ref.shape[1] // 2
    got = got_ref[...].astype(f32)
    third = head_dim // 3
    stats = got[:, half:, :]
    scale = jnp.exp(stats - jnp.max(stats, axis=0, keepdims=True))[:, :, 0:1]
    totals = jnp.sum(scale * stats, axis=0)
    denoms = totals[:, third : third + 1] + totals[:, 2 * third : 2 * third + 1]
    summed = jnp.sum(scale * got[:, :half, :], axis=0)
    attended = (summed / denoms).astype(bf16)
    attended = jnp.concatenate(
        [attended[n : n + seq_count] for n in range(0, half, seq_count)], axis=1
    )
    attended_ref[...] = attended
    other = columns(1 - core, send_ref.shape[1])
    send_ref[...] = jnp.dot(attended, weight_ref[:, other], preferred_element_type=f32)


def keep_kernel(attended_ref, weight_ref, keep_ref):
    core = lax.rem(lax.axis_index("ctx"), 2)
    own = columns(core, keep_ref.shape[1])
    keep_ref[...] = jnp.dot(attended_ref[...], weight_ref[:, own], preferred_element_type=f32)


def spread_kernel(keep_ref, came_ref, out_ref):
    total = (keep_ref[...] + came_ref[...]).astype(out_ref.dtype)
    quarter = out_ref.shape[2]
    for n in range(out_ref.shape[0]):
        out_ref[n] = total[:, n % 2 * quarter : (n % 2 + 1) * quarter]


def resid_kernel(got_ref, hidden_ref, out_ref):
    core = lax.rem(lax.axis_index("ctx"), 2)
    quarter = got_ref.shape[2]
    for side in range(2):
        start = 2 * side * quarter
        hidden = jnp.where(
            core == 0,
            hidden_ref[:, start : start + quarter].astype(f32),
            hidden_ref[:, start + quarter : start + 2 * quarter].astype(f32),
        )
        total = got_ref[side].astype(f32)
        for n in range(side + 2, got_ref.shape[0], 2):
            total = total + got_ref[n].astype(f32)
        out_ref[:, side * quarter : (side + 1) * quarter] = hidden + total


def gated(core, half_ref, gain_ref, weight_refs):
    quarter = half_ref.shape[1] // 2
    acts = [None] * len(weight_refs)
    for side in range(2):
        cols = columns(2 * side + core, quarter)
        rows = half_ref[:, side * quarter : (side + 1) * quarter]
        rows = (rows * gain_ref[:, cols]).astype(bf16)
        for n, weight_ref in enumerate(weight_refs):
            act = dot_nt(rows, weight_ref[:, cols])
            acts[n] = act if side == 0 else acts[n] + act
    return acts


def squares(half_ref):
    return jnp.sum(half_ref[...] * half_ref[...], axis=1, keepdims=True)


def own_half_kernel(mine_ref, gain_ref, gate_ref, up_ref, down_ref, gate_out, up_out):
    del down_ref
    core = lax.rem(lax.axis_index("ctx"), 2)
    gate_out[...], up_out[...] = gated(core, mine_ref, gain_ref, (gate_ref, up_ref))


def expert_kernel(
    mine_ref,
    came_ref,
    gate_part,
    up_part,
    gain_ref,
    gate_ref,
    up_ref,
    down_ref,
    routes_ref,
    share_ref,
    out_ref,
    mine_out,
    resid_ref,
):
    index = lax.axis_index("ctx")
    core = lax.rem(index, 2)
    expert = lax.div(index, QUARTERS)
    quarter = mine_ref.shape[1] // 2
    gate_act, up_act = gated(1 - core, came_ref, gain_ref, (gate_ref, up_ref))
    square = squares(mine_ref) + squares(came_ref)
    inverse_rms = lax.rsqrt(square / (4 * quarter) + eps)
    gate_act = (gate_act + gate_part[...]) * inverse_rms
    up_act = (up_act + up_part[...]) * inverse_rms
    hidden = (gate_act / (1.0 + jnp.exp(-gate_act)) * up_act).astype(bf16)
    for side in range(2):
        cut = slice(side * quarter, (side + 1) * quarter)
        resid_ref[:, columns(2 * side + core, quarter)] = mine_ref[:, cut]
        resid_ref[:, columns(2 * side + 1 - core, quarter)] = came_ref[:, cut]
    col_dev = mine_out.shape[1]
    if col_dev == resid_ref.shape[1]:
        mine_out[...] = resid_ref[...]
    else:
        mine_out[...] = resid_ref[:, columns(index, col_dev)]
    share = jnp.where(routes_ref[...] == expert, share_ref[...], 0.0)
    share = jnp.sum(share, axis=1, keepdims=True)
    out = jnp.dot(hidden, down_ref[...], preferred_element_type=f32)
    out_ref[...] = (out * share).astype(bf16)


def merge_parts(queries, key_cache, value_cache, devices):
    seq_count, head_count, head_dim = queries.shape
    kv_heads = key_cache.shape[2] // head_dim
    local_len = key_cache.shape[1]
    query_view = queries.reshape(seq_count, kv_heads, head_count // kv_heads, head_dim)
    key_view = key_cache.reshape(seq_count, local_len, kv_heads, head_dim)
    value_view = value_cache.reshape(seq_count, local_len, kv_heads, head_dim)
    scores = jnp.einsum(
        "sgjd,scgd->sgjc", query_view, key_view, preferred_element_type=f32
    ) * head_dim ** (-0.5)
    peak = jnp.max(scores, axis=-1)
    numer = jnp.exp(scores - peak[..., None])
    denom = jnp.sum(numer, axis=-1)
    weighted = jnp.einsum(
        "sgjc,scgd->sgjd", numer.astype(bf16), value_view, preferred_element_type=f32
    )
    width = head_count * head_dim // devices
    spread = head_dim // width

    def by_owner(stat):
        return jnp.repeat(stat.reshape(seq_count, head_count), spread, axis=1).T[..., None]

    weighted = weighted.reshape(seq_count, devices, width).transpose(1, 0, 2)
    sent = jnp.concatenate([weighted, by_owner(peak), by_owner(denom)], axis=2)
    got = swap_blocks(sent)
    peaks = got[:, :, width : width + 1]
    scale = jnp.exp(peaks - jnp.max(peaks, axis=0))
    denoms = jnp.sum(scale * got[:, :, width + 1 :], axis=0)
    return (jnp.sum(scale * got[:, :, :width], axis=0) / denoms).astype(bf16)


def swap_blocks(blocks):
    return lax.all_to_all(blocks, "ctx", split_axis=0, concat_axis=0, tiled=True)


def body(
    queries,
    key_cache,
    value_cache,
    out_weight,
    hidden_in,
    norm_gain,
    gate_weight,
    up_weight,
    down_weight,
    routes,
    route_weight,
):
    devices = lax.axis_size("ctx")
    my_index = lax.axis_index("ctx")
    seq_count, head_count, head_dim = queries.shape
    model_width = hidden_in.shape[1]
    mid = model_width // 2
    feat_dev = head_count * head_dim // devices
    half = jax.ShapeDtypeStruct((seq_count, mid), f32)
    if feat_dev % head_dim == 0:
        heads_dev = feat_dev // head_dim
        parts = attend(queries, key_cache, value_cache, devices, heads_dev)
        got = swap_blocks(parts)
        weight = in_vmem(out_weight)
        send, attended = call(
            functools.partial(send_kernel, seq_count),
            (half, jax.ShapeDtypeStruct((seq_count, feat_dev), bf16)),
            count=2,
        )(got, weight)
        keep = call(keep_kernel, half, count=2)(attended, weight)
    else:
        attended = merge_parts(queries, key_cache, value_cache, devices)
        proj = jnp.dot(attended, out_weight, preferred_element_type=f32)
        low, high = proj[:, :mid], proj[:, mid:]
        first = lax.rem(my_index, 2) == 0
        send, keep = jnp.where(first, high, low), jnp.where(first, low, high)
    pairs = [(n, n ^ 1) for n in range(devices)]
    came = lax.ppermute(send, "ctx", pairs)
    spread = call(
        spread_kernel,
        jax.ShapeDtypeStruct((devices, seq_count, mid // 2), bf16),
        count=2,
        flops=LONG,
    )(keep, came)
    mine = call(resid_kernel, half, count=2)(swap_blocks(spread), hidden_in)
    came = lax.ppermute(mine, "ctx", pairs)
    col_dev = model_width // devices
    aligned = col_dev % 128 == 0
    gain = norm_gain.reshape(1, model_width)
    gate, up = in_vmem(gate_weight[0].T), in_vmem(up_weight[0].T)
    down = in_vmem(down_weight[0])
    act = jax.ShapeDtypeStruct((seq_count, gate.shape[0]), f32)
    gate_part, up_part = call(own_half_kernel, (act, act), count=5)(
        mine, gain, gate, up, down
    )
    out, resid_mine = call(
        expert_kernel,
        (
            jax.ShapeDtypeStruct((seq_count, model_width), bf16),
            jax.ShapeDtypeStruct((seq_count, col_dev if aligned else model_width), f32),
        ),
        count=10,
        scratch=(pltpu.VMEM((seq_count, model_width), f32),),
    )(
        mine,
        came,
        gate_part,
        up_part,
        gain,
        gate,
        up,
        down,
        routes,
        route_weight,
    )
    blocks = lax.all_to_all(
        out.reshape(seq_count, devices, col_dev), "ctx", split_axis=1, concat_axis=1, tiled=True
    )
    if not aligned:
        resid_mine = lax.dynamic_slice_in_dim(resid_mine, my_index * col_dev, col_dev, 1)
    return resid_mine + jnp.sum(blocks.astype(f32), axis=1)


def solution(mesh):
    in_specs = (
        P("group", None, None),
        P("group", "ctx", None),
        P("group", "ctx", None),
        P("ctx", None),
        P("group", None),
        P(),
        P("ctx", None, None),
        P("ctx", None, None),
        P("ctx", None, None),
        P("group", None),
        P("group", None),
    )
    out_specs = P("group", "ctx")
    return jax.shard_map(body, mesh=mesh, in_specs=in_specs, out_specs=out_specs, check_vma=False)
```

```python
import functools

import jax
import jax.numpy as jnp
from jax import lax
from jax.experimental import pallas as pl
from jax.experimental.pallas import tpu as pltpu
from jax.sharding import PartitionSpec as P

QUARTERS = 8


eps = 1e-06
LIMIT = 16 << 20
LONG = 1 << 34
f32 = jnp.float32
bf16 = jnp.bfloat16


def in_vmem(array):
    return pltpu.with_memory_space_constraint(array, pltpu.VMEM)


def in_hbm(array):
    return pltpu.with_memory_space_constraint(array, pltpu.HBM)


def call(kernel, out_shape, in_specs=None, count=0, scratch=(), flops=1 << 10, moved=1 << 10):
    vmem = pl.BlockSpec(memory_space=pltpu.VMEM)
    many = isinstance(out_shape, (tuple, list))
    return pl.pallas_call(
        kernel,
        out_shape=out_shape,
        in_specs=in_specs or [vmem] * count,
        out_specs=[vmem] * len(out_shape) if many else vmem,
        scratch_shapes=list(scratch),
        compiler_params=pltpu.CompilerParams(vmem_limit_bytes=LIMIT),
        cost_estimate=pl.CostEstimate(flops=flops, bytes_accessed=moved, transcendentals=0),
    )


def dot_nt(a, b):
    return lax.dot_general(a, b, (((1,), (1,)), ((), ())), preferred_element_type=f32)


def rows_of(heads_dev, seq_count, owners):
    half = seq_count * heads_dev
    row = lax.broadcasted_iota(jnp.int32, (owners * 2 * half, 1), 0)
    within = lax.rem(row, half)
    seq_of = lax.rem(within, seq_count)
    head_of = lax.div(row, 2 * half) * heads_dev + lax.div(within, seq_count)
    return seq_of, head_of, lax.rem(row, 2 * half) < half


def score_kernel(
    heads_dev, kv_heads, q_hbm, k_hbm, v_hbm, numer_ref, stat_ref, v_ref, q, k, sems
):
    seq_count, local_len, _ = k.shape
    head_dim = q.shape[1]
    head_count = q.shape[0] // seq_count
    moves = ((k_hbm, k), (q_hbm, q), (v_hbm, v_ref))
    copies = [pltpu.make_async_copy(src, dst, sems.at[n]) for n, (src, dst) in enumerate(moves)]
    for copy in copies:
        copy.start()
    owners = head_count // kv_heads // heads_dev
    seq_of, head_of, _ = rows_of(heads_dev, seq_count, owners)
    rows = seq_of.shape[0]
    source = seq_of * head_count + head_of
    column = lax.broadcasted_iota(jnp.int32, (rows, q.shape[0]), 1)
    picks = [
        jnp.where(column == source + g * owners * heads_dev, 1.0, 0.0).astype(bf16)
        for g in range(kv_heads)
    ]
    lane = lax.broadcasted_iota(jnp.int32, (rows, head_dim), 1)
    third = head_dim // 3

    def by_seq(values):
        return jnp.concatenate(
            [jnp.where(seq_of == s, values, 0.0).astype(bf16) for s in range(seq_count)], axis=1
        )

    copies[1].wait()
    queries = [by_seq(jnp.dot(pick, q[...], preferred_element_type=f32)) for pick in picks]
    copies[0].wait()
    copies[2].wait()
    for g in range(kv_heads):
        cut = slice(g * head_dim, (g + 1) * head_dim)
        keys = jnp.concatenate([k[s, :, cut] for s in range(seq_count)], axis=1)
        scores = dot_nt(queries[g], keys) * head_dim ** (-0.5)
        peak = jnp.max(scores, axis=1, keepdims=True).astype(bf16).astype(f32)
        numer = jnp.exp(scores - peak)
        denom = jnp.sum(numer, axis=1, keepdims=True)
        coarse = denom.astype(bf16).astype(f32)
        totals = jnp.where(lane < 2 * third, coarse, denom - coarse)
        stat_ref[g * rows : (g + 1) * rows] = jnp.where(lane < third, peak, totals)
        numer_ref[g * rows : (g + 1) * rows] = by_seq(numer)


def value_kernel(heads_dev, kv_heads, numer_ref, stat_ref, v_ref, out_ref):
    seq_count = v_ref.shape[0]
    head_dim = stat_ref.shape[1]
    owners = out_ref.shape[0] // kv_heads
    _, _, is_part = rows_of(heads_dev, seq_count, owners)
    rows = is_part.shape[0]
    for g in range(kv_heads):
        cut = slice(g * head_dim, (g + 1) * head_dim)
        own = slice(g * rows, (g + 1) * rows)
        values = jnp.concatenate([v_ref[s, :, cut] for s in range(seq_count)], axis=0)
        part = jnp.dot(numer_ref[own], values, preferred_element_type=f32)
        block = jnp.where(is_part, part, stat_ref[own]).astype(bf16)
        out_ref[g * owners : (g + 1) * owners] = block.reshape(owners, -1, head_dim)


def attend(queries, key_cache, value_cache, devices, heads_dev):
    seq_count, head_count, head_dim = queries.shape
    kv_heads = key_cache.shape[2] // head_dim
    hbm = pl.BlockSpec(memory_space=pltpu.HBM)
    q = queries.reshape(seq_count * head_count, head_dim)
    rows = 2 * q.shape[0]
    numers, stats, values = call(
        functools.partial(score_kernel, heads_dev, kv_heads),
        (
            pltpu.VMEM((rows, seq_count * key_cache.shape[1]), bf16),
            pltpu.VMEM((rows, head_dim), f32),
            pltpu.VMEM(value_cache.shape, bf16),
        ),
        in_specs=[hbm] * 3,
        scratch=(
            pltpu.VMEM(q.shape, bf16),
            pltpu.VMEM(key_cache.shape, bf16),
            pltpu.SemaphoreType.DMA((3,)),
        ),
    )(in_hbm(q), in_hbm(key_cache), in_hbm(value_cache))
    return call(
        functools.partial(value_kernel, heads_dev, kv_heads),
        pltpu.VMEM((devices, 2 * seq_count * heads_dev, head_dim), bf16),
        count=3,
        flops=LONG,
    )(numers, stats, values)


def columns(block, width):
    return pl.ds(pl.multiple_of(block * width, width), width)


def send_kernel(seq_count, got_ref, weight_ref, send_ref, attended_ref):
    core = lax.rem(lax.axis_index("ctx"), 2)
    head_dim = got_ref.shape[2]
    half = got_ref.shape[1] // 2
    got = got_ref[...].astype(f32)
    third = head_dim // 3
    stats = got[:, half:, :]
    scale = jnp.exp(stats - jnp.max(stats, axis=0, keepdims=True))[:, :, 0:1]
    totals = jnp.sum(scale * stats, axis=0)
    denoms = totals[:, third : third + 1] + totals[:, 2 * third : 2 * third + 1]
    summed = jnp.sum(scale * got[:, :half, :], axis=0)
    attended = (summed / denoms).astype(bf16)
    attended = jnp.concatenate(
        [attended[n : n + seq_count] for n in range(0, half, seq_count)], axis=1
    )
    attended_ref[...] = attended
    other = columns(1 - core, send_ref.shape[1])
    send_ref[...] = jnp.dot(attended, weight_ref[:, other], preferred_element_type=f32)


def keep_kernel(attended_ref, weight_ref, keep_ref):
    core = lax.rem(lax.axis_index("ctx"), 2)
    own = columns(core, keep_ref.shape[1])
    keep_ref[...] = jnp.dot(attended_ref[...], weight_ref[:, own], preferred_element_type=f32)


def spread_kernel(keep_ref, came_ref, out_ref):
    total = (keep_ref[...] + came_ref[...]).astype(out_ref.dtype)
    quarter = out_ref.shape[2]
    for n in range(out_ref.shape[0]):
        out_ref[n] = total[:, n % 2 * quarter : (n % 2 + 1) * quarter]


def resid_kernel(got_ref, hidden_ref, out_ref):
    core = lax.rem(lax.axis_index("ctx"), 2)
    quarter = got_ref.shape[2]
    for side in range(2):
        start = 2 * side * quarter
        hidden = jnp.where(
            core == 0,
            hidden_ref[:, start : start + quarter].astype(f32),
            hidden_ref[:, start + quarter : start + 2 * quarter].astype(f32),
        )
        total = got_ref[side].astype(f32)
        for n in range(side + 2, got_ref.shape[0], 2):
            total = total + got_ref[n].astype(f32)
        out_ref[:, side * quarter : (side + 1) * quarter] = hidden + total


def gated(core, half_ref, gain_ref, weight_refs):
    quarter = half_ref.shape[1] // 2
    acts = [None] * len(weight_refs)
    for side in range(2):
        cols = columns(2 * side + core, quarter)
        rows = half_ref[:, side * quarter : (side + 1) * quarter]
        rows = (rows * gain_ref[:, cols]).astype(bf16)
        for n, weight_ref in enumerate(weight_refs):
            act = dot_nt(rows, weight_ref[:, cols])
            acts[n] = act if side == 0 else acts[n] + act
    return acts


def squares(half_ref):
    return jnp.sum(half_ref[...] * half_ref[...], axis=1, keepdims=True)


def own_half_kernel(mine_ref, gain_ref, gate_ref, up_ref, down_ref, gate_out, up_out):
    del down_ref
    core = lax.rem(lax.axis_index("ctx"), 2)
    gate_out[...], up_out[...] = gated(core, mine_ref, gain_ref, (gate_ref, up_ref))


def expert_kernel(
    mine_ref,
    came_ref,
    gate_part,
    up_part,
    gain_ref,
    gate_ref,
    up_ref,
    down_ref,
    routes_ref,
    share_ref,
    out_ref,
    mine_out,
    resid_ref,
):
    index = lax.axis_index("ctx")
    core = lax.rem(index, 2)
    expert = lax.div(index, QUARTERS)
    quarter = mine_ref.shape[1] // 2
    gate_act, up_act = gated(1 - core, came_ref, gain_ref, (gate_ref, up_ref))
    square = squares(mine_ref) + squares(came_ref)
    inverse_rms = lax.rsqrt(square / (4 * quarter) + eps)
    gate_act = (gate_act + gate_part[...]) * inverse_rms
    up_act = (up_act + up_part[...]) * inverse_rms
    hidden = (gate_act / (1.0 + jnp.exp(-gate_act)) * up_act).astype(bf16)
    for side in range(2):
        cut = slice(side * quarter, (side + 1) * quarter)
        resid_ref[:, columns(2 * side + core, quarter)] = mine_ref[:, cut]
        resid_ref[:, columns(2 * side + 1 - core, quarter)] = came_ref[:, cut]
    col_dev = mine_out.shape[1]
    if col_dev == resid_ref.shape[1]:
        mine_out[...] = resid_ref[...]
    else:
        mine_out[...] = resid_ref[:, columns(index, col_dev)]
    share = jnp.where(routes_ref[...] == expert, share_ref[...], 0.0)
    share = jnp.sum(share, axis=1, keepdims=True)
    out = jnp.dot(hidden, down_ref[...], preferred_element_type=f32)
    out_ref[...] = (out * share).astype(bf16)


def merge_parts(queries, key_cache, value_cache, devices):
    seq_count, head_count, head_dim = queries.shape
    kv_heads = key_cache.shape[2] // head_dim
    local_len = key_cache.shape[1]
    query_view = queries.reshape(seq_count, kv_heads, head_count // kv_heads, head_dim)
    key_view = key_cache.reshape(seq_count, local_len, kv_heads, head_dim)
    value_view = value_cache.reshape(seq_count, local_len, kv_heads, head_dim)
    scores = jnp.einsum(
        "sgjd,scgd->sgjc", query_view, key_view, preferred_element_type=f32
    ) * head_dim ** (-0.5)
    peak = jnp.max(scores, axis=-1)
    numer = jnp.exp(scores - peak[..., None])
    denom = jnp.sum(numer, axis=-1)
    weighted = jnp.einsum(
        "sgjc,scgd->sgjd", numer.astype(bf16), value_view, preferred_element_type=f32
    )
    width = head_count * head_dim // devices
    spread = head_dim // width

    def by_owner(stat):
        return jnp.repeat(stat.reshape(seq_count, head_count), spread, axis=1).T[..., None]

    weighted = weighted.reshape(seq_count, devices, width).transpose(1, 0, 2)
    sent = jnp.concatenate([weighted, by_owner(peak), by_owner(denom)], axis=2)
    got = swap_blocks(sent)
    peaks = got[:, :, width : width + 1]
    scale = jnp.exp(peaks - jnp.max(peaks, axis=0))
    denoms = jnp.sum(scale * got[:, :, width + 1 :], axis=0)
    return (jnp.sum(scale * got[:, :, :width], axis=0) / denoms).astype(bf16)


def swap_blocks(blocks):
    return lax.all_to_all(blocks, "ctx", split_axis=0, concat_axis=0, tiled=True)


def body(
    queries,
    key_cache,
    value_cache,
    out_weight,
    hidden_in,
    norm_gain,
    gate_weight,
    up_weight,
    down_weight,
    routes,
    route_weight,
):
    devices = lax.axis_size("ctx")
    my_index = lax.axis_index("ctx")
    seq_count, head_count, head_dim = queries.shape
    model_width = hidden_in.shape[1]
    mid = model_width // 2
    feat_dev = head_count * head_dim // devices
    half = jax.ShapeDtypeStruct((seq_count, mid), f32)
    if feat_dev % head_dim == 0:
        heads_dev = feat_dev // head_dim
        parts = attend(queries, key_cache, value_cache, devices, heads_dev)
        got = swap_blocks(parts)
        weight = in_vmem(out_weight)
        send, attended = call(
            functools.partial(send_kernel, seq_count),
            (half, jax.ShapeDtypeStruct((seq_count, feat_dev), bf16)),
            count=2,
        )(got, weight)
        keep = call(keep_kernel, half, count=2)(attended, weight)
    else:
        attended = merge_parts(queries, key_cache, value_cache, devices)
        proj = jnp.dot(attended, out_weight, preferred_element_type=f32)
        low, high = proj[:, :mid], proj[:, mid:]
        first = lax.rem(my_index, 2) == 0
        send, keep = jnp.where(first, high, low), jnp.where(first, low, high)
    pairs = [(n, n ^ 1) for n in range(devices)]
    came = lax.ppermute(send, "ctx", pairs)
    spread = call(
        spread_kernel,
        jax.ShapeDtypeStruct((devices, seq_count, mid // 2), bf16),
        count=2,
    )(keep, came)
    mine = call(resid_kernel, half, count=2)(swap_blocks(spread), hidden_in)
    came = lax.ppermute(mine, "ctx", pairs)
    col_dev = model_width // devices
    aligned = col_dev % 128 == 0
    gain = norm_gain.reshape(1, model_width)
    gate, up = in_vmem(gate_weight[0].T), in_vmem(up_weight[0].T)
    down = in_vmem(down_weight[0])
    act = jax.ShapeDtypeStruct((seq_count, gate.shape[0]), f32)
    gate_part, up_part = call(own_half_kernel, (act, act), count=5)(
        mine, gain, gate, up, down
    )
    out, resid_mine = call(
        expert_kernel,
        (
            jax.ShapeDtypeStruct((seq_count, model_width), bf16),
            jax.ShapeDtypeStruct((seq_count, col_dev if aligned else model_width), f32),
        ),
        count=10,
        scratch=(pltpu.VMEM((seq_count, model_width), f32),),
    )(
        mine,
        came,
        gate_part,
        up_part,
        gain,
        gate,
        up,
        down,
        routes,
        route_weight,
    )
    blocks = lax.all_to_all(
        out.reshape(seq_count, devices, col_dev), "ctx", split_axis=1, concat_axis=1, tiled=True
    )
    if not aligned:
        resid_mine = lax.dynamic_slice_in_dim(resid_mine, my_index * col_dev, col_dev, 1)
    return resid_mine + jnp.sum(blocks.astype(f32), axis=1)


def solution(mesh):
    in_specs = (
        P("group", None, None),
        P("group", "ctx", None),
        P("group", "ctx", None),
        P("ctx", None),
        P("group", None),
        P(),
        P("ctx", None, None),
        P("ctx", None, None),
        P("ctx", None, None),
        P("group", None),
        P("group", None),
    )
    out_specs = P("group", "ctx")
    return jax.shard_map(body, mesh=mesh, in_specs=in_specs, out_specs=out_specs, check_vma=False)
```
